32 devices in a mesh: dp: 4 (over y, x), fsdp: 8 (over z, core).
Axes of the slice: x: 2, y: 2, z: 4, core: 2. Of those that a mesh axis runs over, the one named last changes fastest.
Arguments:
- hidden_in: bfloat16 [32, 8192], P(('dp', 'fsdp')), may hold values from -6 to 6
- lengths: int32 [32], P(('dp', 'fsdp')), may hold values from 1 to 511
- key_cache: bfloat16 [32, 512, 1024], P(('dp', 'fsdp')), may hold values from -68 to 68
- value_cache: bfloat16 [32, 512, 1024], P(('dp', 'fsdp')), may hold values from -6 to 6
- attn_gain: bfloat16 [8192], replicated, may hold values from 0.5 to 1.5
- w_qkv: bfloat16 [8192, 10240], P('fsdp', 'dp'), may hold values from -0.0625 to 0.0625
- w_out: bfloat16 [8192, 8192], P('fsdp', 'dp'), may hold values from -0.5 to 0.5
- mlp_gain: bfloat16 [8192], replicated, may hold values from 0.5 to 1.5
- w_gate: bfloat16 [8192, 28672], P('dp', 'fsdp'), may hold values from -0.0625 to 0.0625
- w_up: bfloat16 [8192, 28672], P('dp', 'fsdp'), may hold values from -0.0625 to 0.0625
- w_down: bfloat16 [28672, 8192], P('fsdp', 'dp'), may hold values from -0.03125 to 0.03125
Outputs:
- hidden_out: bfloat16 [32, 8192], P(('dp', 'fsdp'))
- new_keys: bfloat16 [32, 1024], P(('dp', 'fsdp'))
- new_values: bfloat16 [32, 1024], P(('dp', 'fsdp'))
The draws below stay inside these ranges and needn't reach their ends.
Inputs may be any that keep to these rules, and one draw needn't show every extreme that they name: Each sequence's number of cached positions; its new token takes position lengths.
All inputs are finite; a program needn't handle non-finite values.
Results may differ from the reference program's by a relative error of at most 0.012.
The reference program's roundings to bfloat16 on the way (of `normed`, `queries`, `probability`, `mixed`, `normed_mid` and `activated`) count: a program that leaves them out, or rounds other values in their place, can miss the bound.
Values may be sent and summed in bfloat16 or wider, within the bound.
A program may use at most 128 MiB of HBM per device.

```python
import jax
import jax.numpy as jnp
from jax import lax

D = 8192
HEADS = 64
KV_HEADS = 8
HD = 128
FF = 28672
CTX = 512
TOKENS = 32


def draw_key_cache(key, part):
    shape = (TOKENS, CTX, KV_HEADS * HD)
    base_key, pick_key = jax.random.split(jax.random.fold_in(key, 17))
    values = jnp.clip(jax.random.normal(base_key, shape, jnp.float32), -6.0, 6.0)
    return values.astype(jnp.bfloat16)


def with_ends(values, rng, least, high):
    dims = values.shape
    index_at = [jax.random.randint(jax.random.fold_in(rng, axis), (), 0, dims[axis]) for axis in range(len(dims))]
    values = values.at[tuple(index_at)].set(least)
    longest = dims.index(max(dims))
    index_at[longest] = (index_at[longest] + 1) % dims[longest]
    return values.at[tuple(index_at)].set(high)


def block_scale(own_key, dims, shards, smallest, top_value):
    loudness = 1.0
    for position, parts in shards:
        draws = jax.random.uniform(jax.random.fold_in(jax.random.fold_in(own_key, 6), position), (parts,), jnp.float32, smallest / len(shards), top_value / len(shards))
        loudness = loudness * jnp.repeat(jnp.exp(draws), dims[position] // parts).reshape((-1,) + (1,) * (len(dims) - 1 - position))
    return loudness


def scatter_about(rng, dims, width, most, cuts=(), kind=jnp.bfloat16):
    level = block_scale(rng, dims, cuts, -0.22, 0.18) if cuts else 1.0
    array = jax.random.normal(rng, dims, jnp.float32) * width * level
    return jnp.minimum(jnp.maximum(array, -most), most).astype(kind)


def setup_inputs(seed: int = 0) -> dict:
    splits = jax.random.split(jax.random.key(seed), 12)
    hidden_in = scatter_about(splits[0], (TOKENS, D), 1.0, 6.0, ((0, 32),))
    lengths = with_ends(jax.random.randint(splits[1], (TOKENS,), 1, CTX), jax.random.fold_in(splits[1], 1), 1, CTX - 1).astype(jnp.int32)
    key_cache = draw_key_cache(jax.random.fold_in(splits[11], 71), 0)
    value_cache = scatter_about(splits[3], (TOKENS, CTX, KV_HEADS * HD), 1.0, 6.0, ((0, 32),))
    attn_gain = jnp.clip(1.0 + 0.1 * jax.random.normal(splits[4], (D,), jnp.float32), 0.5, 1.5).astype(jnp.bfloat16)
    w_qkv = scatter_about(splits[5], (D, (HEADS + 2 * KV_HEADS) * HD), D ** -0.5, 0.0625, ((0, 8), (1, 4)))
    w_out = scatter_about(splits[6], (HEADS * HD, D), HD ** -0.5, 0.5, ((0, 8), (1, 4)))
    mlp_gain = jnp.clip(1.0 + 0.1 * jax.random.normal(splits[7], (D,), jnp.float32), 0.5, 1.5).astype(jnp.bfloat16)
    w_gate = scatter_about(splits[8], (D, FF), D ** -0.5, 0.0625, ((0, 4), (1, 8)))
    w_up = scatter_about(splits[9], (D, FF), D ** -0.5, 0.0625, ((0, 4), (1, 8)))
    w_down = scatter_about(splits[10], (FF, D), FF ** -0.5, 0.03125, ((0, 8), (1, 4)))
    return {"hidden_in": hidden_in, "lengths": lengths, "key_cache": key_cache, "value_cache": value_cache, "attn_gain": attn_gain, "w_qkv": w_qkv, "w_out": w_out, "mlp_gain": mlp_gain, "w_gate": w_gate, "w_up": w_up, "w_down": w_down}


rope_base = 500000.0
norm_eps = 1e-05

def rms_scale(values, gain_row):
    mean_square = lax.optimization_barrier(jnp.mean(values * values, axis=-1, keepdims=True))
    return values * lax.rsqrt(mean_square + norm_eps) * gain_row.astype(jnp.float32)

def rotate(values, positions):
    half_dim = values.shape[-1] // 2
    frequency = rope_base ** (-2.0 * jnp.arange(half_dim, dtype=jnp.float32) / values.shape[-1])
    angles = positions.astype(jnp.float32)[:, None] * frequency[None, :]
    cosine = jnp.cos(angles)[:, None, :]
    sine_wave = jnp.sin(angles)[:, None, :]
    lower_half = values[..., :half_dim]
    upper_half = values[..., half_dim:]
    return jnp.concatenate([lower_half * cosine - upper_half * sine_wave, upper_half * cosine + lower_half * sine_wave], axis=-1)

def attend_one(arguments):
    queries, new_keys, new_values, key_rows, value_rows, length = arguments
    context = key_rows.shape[0]
    score_scale = HD ** (-0.5)
    grouped = queries.astype(jnp.float32).reshape(KV_HEADS, HEADS // KV_HEADS, HD)
    key_float = key_rows.astype(jnp.float32).reshape(context, KV_HEADS, HD)
    value_float = value_rows.astype(jnp.float32).reshape(context, KV_HEADS, HD)
    scores = jnp.einsum('kgd,ckd->kgc', grouped, key_float) * score_scale
    is_valid = jnp.arange(context, dtype=jnp.int32)[None, None, :] < length
    scores = jnp.where(is_valid, scores, -1e+30)
    own_score = jnp.einsum('kgd,kd->kg', grouped, new_keys.astype(jnp.float32)) * score_scale
    row_max = jnp.maximum(lax.optimization_barrier(jnp.max(scores, axis=-1)), own_score)
    weights = jnp.exp(scores - row_max[..., None])
    own_weight = jnp.exp(own_score - row_max)
    denom_sum = lax.optimization_barrier(jnp.sum(weights, axis=-1)) + own_weight
    probability = (weights / denom_sum[..., None]).astype(jnp.bfloat16).astype(jnp.float32)
    own_prob = (own_weight / denom_sum).astype(jnp.bfloat16).astype(jnp.float32)
    mixed = jnp.einsum('kgc,ckd->kgd', probability, value_float)
    mixed = mixed + own_prob[..., None] * new_values.astype(jnp.float32)[:, None, :]
    return mixed.astype(jnp.bfloat16).reshape(HEADS * HD)

def reference(hidden_in, lengths, key_cache, value_cache, attn_gain, w_qkv, w_out, mlp_gain, w_gate, w_up, w_down):
    q_width = HEADS * HD
    kv_width = KV_HEADS * HD
    residual = hidden_in.astype(jnp.float32)
    normed = rms_scale(residual, attn_gain).astype(jnp.bfloat16)
    projected = jnp.dot(normed, w_qkv, preferred_element_type=jnp.float32)
    token_count = projected.shape[0]
    queries = rotate(projected[:, :q_width].reshape(token_count, HEADS, HD), lengths).astype(jnp.bfloat16)
    new_keys = rotate(projected[:, q_width:q_width + kv_width].reshape(token_count, KV_HEADS, HD), lengths).astype(jnp.bfloat16)
    new_values = projected[:, q_width + kv_width:].astype(jnp.bfloat16)
    mixed = lax.map(attend_one, (queries, new_keys, new_values.reshape(token_count, KV_HEADS, HD), key_cache, value_cache, lengths))
    residual_mid = residual + jnp.dot(mixed, w_out, preferred_element_type=jnp.float32)
    normed_mid = rms_scale(residual_mid, mlp_gain).astype(jnp.bfloat16)
    gate_sum = jnp.dot(normed_mid, w_gate, preferred_element_type=jnp.float32)
    up_sum = jnp.dot(normed_mid, w_up, preferred_element_type=jnp.float32)
    activated = (jax.nn.silu(gate_sum) * up_sum).astype(jnp.bfloat16)
    down_sum = jnp.dot(activated, w_down, preferred_element_type=jnp.float32)
    hidden_out = (residual_mid + down_sum).astype(jnp.bfloat16)
    return (hidden_out, new_keys.reshape(token_count, kv_width), new_values)
```

```python
import functools

import jax
import jax.numpy as jnp
from jax import lax
from jax.experimental import pallas as pl
from jax.experimental.pallas import tpu as pltpu
from jax.sharding import PartitionSpec as P

HEADS = 64
KV_HEADS = 8
HD = 128


rope_base = 500000.0
norm_eps = 1e-05


def rms_scale(values, gain_row):
    mean_square = jnp.mean(values * values, axis=-1, keepdims=True)
    return values * lax.rsqrt(mean_square + norm_eps) * gain_row.astype(jnp.float32)


def rotate(values, positions):
    half_dim = values.shape[-1] // 2
    frequency = rope_base ** (-2.0 * jnp.arange(half_dim, dtype=jnp.float32) / values.shape[-1])
    angles = positions.astype(jnp.float32)[:, None] * frequency[None, :]
    cosine = jnp.cos(angles)[:, None, :]
    sine_wave = jnp.sin(angles)[:, None, :]
    lower_half = values[..., :half_dim]
    upper_half = values[..., half_dim:]
    return jnp.concatenate(
        [
            lower_half * cosine - upper_half * sine_wave,
            upper_half * cosine + lower_half * sine_wave,
        ],
        axis=-1,
    )


def attend(queries, new_keys, new_values, key_cache, value_cache, lengths):
    seq_count, context, kv_width = key_cache.shape
    kv_heads = new_keys.shape[1]
    head_dim = new_keys.shape[2]
    score_scale = head_dim ** (-0.5)
    key_rows = key_cache.reshape(seq_count, context, kv_heads, head_dim)
    value_rows = value_cache.reshape(seq_count, context, kv_heads, head_dim)
    grouped = queries.reshape(seq_count, kv_heads, -1, head_dim)
    scores = (
        jnp.einsum("skgd,sckd->skgc", grouped, key_rows, preferred_element_type=jnp.float32)
        * score_scale
    )
    is_valid = (
        jnp.arange(context, dtype=jnp.int32)[None, None, None, :] < lengths[:, None, None, None]
    )
    scores = jnp.where(is_valid, scores, -1e30)
    own_score = (
        jnp.einsum("skgd,skd->skg", grouped, new_keys, preferred_element_type=jnp.float32)
        * score_scale
    )
    row_max = jnp.maximum(jnp.max(scores, axis=-1), own_score)
    weights = jnp.exp(scores - row_max[..., None])
    own_weight = jnp.exp(own_score - row_max)
    denom_sum = jnp.sum(weights, axis=-1) + own_weight
    probability = (weights / denom_sum[..., None]).astype(jnp.bfloat16)
    own_prob = (own_weight / denom_sum).astype(jnp.bfloat16)
    mixed = jnp.einsum(
        "skgc,sckd->skgd", probability, value_rows, preferred_element_type=jnp.float32
    )
    mixed = (
        mixed
        + own_prob.astype(jnp.float32)[..., None] * new_values.astype(jnp.float32)[:, :, None, :]
    )
    return mixed.astype(jnp.bfloat16).reshape(seq_count, -1)


def spread_project(rows, weight):
    block = lax.all_to_all(rows[None], "fsdp", split_axis=2, concat_axis=0, tiled=True)
    block = lax.all_gather(block, "dp", axis=0)
    partial_sum = jnp.einsum("afsk,kn->afsn", block, weight, preferred_element_type=jnp.float32)
    share = lax.psum_scatter(partial_sum, "fsdp", scatter_dimension=1, tiled=True)
    moved = lax.all_to_all(share, "dp", split_axis=0, concat_axis=3, tiled=True)
    return moved[0, 0]


def on_device_plain(
    hidden_in,
    lengths,
    key_cache,
    value_cache,
    attn_gain,
    w_qkv,
    w_out,
    mlp_gain,
    w_gate,
    w_up,
    w_down,
):
    seq_count = hidden_in.shape[0]
    q_width = HEADS * HD
    kv_width = KV_HEADS * HD
    residual = hidden_in.astype(jnp.float32)
    normed = rms_scale(residual, attn_gain).astype(jnp.bfloat16)
    projected = spread_project(normed, w_qkv)
    queries = rotate(projected[:, :q_width].reshape(seq_count, HEADS, HD), lengths).astype(
        jnp.bfloat16
    )
    new_keys = rotate(
        projected[:, q_width : q_width + kv_width].reshape(seq_count, KV_HEADS, HD), lengths
    ).astype(jnp.bfloat16)
    new_values = projected[:, q_width + kv_width :].astype(jnp.bfloat16)
    mixed = attend(
        queries,
        new_keys,
        new_values.reshape(seq_count, KV_HEADS, HD),
        key_cache,
        value_cache,
        lengths,
    )
    attn_sum = spread_project(mixed, w_out)
    residual_mid = residual + attn_sum
    normed_mid = rms_scale(residual_mid, mlp_gain).astype(jnp.bfloat16)
    mlp_in = lax.all_to_all(normed_mid[None], "dp", split_axis=2, concat_axis=0, tiled=True)
    pieces = lax.all_gather(mlp_in[None], "fsdp", axis=0, tiled=True)
    gate_part = jnp.einsum("fask,kn->fasn", pieces, w_gate, preferred_element_type=jnp.float32)
    up_part = jnp.einsum("fask,kn->fasn", pieces, w_up, preferred_element_type=jnp.float32)
    partials = jnp.stack([gate_part, up_part], axis=3)
    summed = lax.psum(partials.astype(jnp.bfloat16), "dp").astype(jnp.float32)
    activated = (jax.nn.silu(summed[:, :, :, 0]) * summed[:, :, :, 1]).astype(jnp.bfloat16)
    reduced_down = lax.psum_scatter(
        jnp.einsum("fask,kn->fasn", activated, w_down, preferred_element_type=jnp.float32),
        "fsdp",
        scatter_dimension=0,
        tiled=True,
    )
    down_sum = lax.all_to_all(
        reduced_down.astype(jnp.bfloat16), "dp", split_axis=1, concat_axis=3, tiled=True
    ).astype(reduced_down.dtype)[0, 0]
    hidden_out = (residual_mid + down_sum).astype(jnp.bfloat16)
    return (hidden_out, new_keys.reshape(seq_count, kv_width), new_values)


LANES = 128
MESH = pl.DeviceIdType.MESH
F32 = jnp.float32
BF16 = jnp.bfloat16


def rms_tile(values, gain):
    total = jnp.sum(jnp.sum(values * values, axis=1, keepdims=True), axis=0, keepdims=True)
    return values * lax.rsqrt(total / values.size + norm_eps) * gain.astype(F32)


def gather_features(ref, tokens, rows):
    pieces = [ref[pl.ds(r, tokens, stride=rows), :] for r in range(rows)]
    return jnp.concatenate(pieces, axis=1).astype(BF16)


def layer_kernel(
    dp_size,
    fsdp_size,
    pitch,
    len_ref,
    hid_ref,
    cos_ref,
    sin_ref,
    attn_gain_ref,
    mlp_gain_ref,
    key_hbm,
    value_hbm,
    qkv_hbm,
    out_hbm,
    gate_hbm,
    up_hbm,
    down_hbm,
    hidden_ref,
    keys_ref,
    values_ref,
    w_qkv,
    w_out,
    w_gate,
    w_up,
    w_down,
    key_buf,
    value_buf,
    a_send,
    a_recv,
    b_send,
    b_recv,
    heads_buf,
    c_send,
    c_recv,
    d_send,
    d_recv,
    mid_buf,
    e_send,
    e_recv,
    x_buf,
    f_send,
    f_recv,
    act_buf,
    h_send,
    h_recv,
    load_sem,
    send_sem,
    recv_sem,
):
    devices = dp_size * fsdp_size
    my_dp = lax.axis_index("dp")
    my_fsdp = lax.axis_index("fsdp")
    me = my_dp * fsdp_size + my_fsdp

    loads = [
        pltpu.make_async_copy(source, target, load_sem.at[i])
        for i, (source, target) in enumerate(
            (
                (qkv_hbm, w_qkv),
                (key_hbm.at[0], key_buf),
                (value_hbm.at[0], value_buf),
                (out_hbm, w_out),
                (gate_hbm, w_gate),
                (up_hbm, w_up),
                (down_hbm, w_down),
            )
        )
    ]
    loads[0].start()

    def place(step):
        other = lax.rem(me + step, devices)
        return other, other // fsdp_size, lax.rem(other, fsdp_size)

    barrier = pltpu.get_barrier_semaphore()

    @pl.loop(1, devices)
    def _(step):
        _, dp_at, fsdp_at = place(step)
        pl.semaphore_signal(barrier, inc=1, device_id=(dp_at, fsdp_at), device_id_type=MESH)

    def exchange(phase, source, target, rows, offset):
        mine = pl.ds(pl.multiple_of(me * rows, 8), rows)

        @pl.loop(1, devices)
        def _(step):
            other, dp_at, fsdp_at = place(step)
            start = pl.multiple_of(offset(other, dp_at, fsdp_at) * rows, 8)
            pltpu.make_async_remote_copy(
                src_ref=source.at[pl.ds(start, rows)],
                dst_ref=target.at[mine],
                send_sem=send_sem.at[phase],
                recv_sem=recv_sem.at[phase],
                device_id=(dp_at, fsdp_at),
                device_id_type=MESH,
            ).start()

        own = pl.multiple_of(offset(me, my_dp, my_fsdp) * rows, 8)
        target[mine, :] = source[pl.ds(own, rows), :]

    def wait_all(sem, target, rows):
        whole = target.at[pl.ds(0, (devices - 1) * rows)]
        pltpu.make_async_copy(whole, whole, sem).wait()

    def by_fsdp(other, dp_at, fsdp_at):
        return fsdp_at

    def by_dp(other, dp_at, fsdp_at):
        return dp_at

    def by_token(other, dp_at, fsdp_at):
        return other

    def project(x, weight, target, width, step_pitch):
        chunk = 512

        @pl.loop(0, width // chunk)
        def _(c):
            columns = pl.ds(pl.multiple_of(c * chunk, chunk), chunk)
            result = jnp.dot(x[...], weight[:, columns], preferred_element_type=F32)
            for j in range(chunk // LANES):
                row = c * (chunk // LANES) + j
                target[pl.ds(row, devices, stride=step_pitch), :] = result[
                    :, j * LANES : (j + 1) * LANES
                ]

    def sum_block(ref, dp_at, rows, used):
        total = None
        for f in range(fsdp_size):
            start = (dp_at * fsdp_size + f) * rows
            piece = ref[start : start + used, :]
            total = piece if total is None else total + piece
        return total

    residual = hid_ref[...].astype(F32)
    normed = rms_tile(residual, attn_gain_ref[...])
    a_send[...] = normed.astype(BF16).astype(F32)
    row_tiles = a_recv.shape[0] // devices
    pl.semaphore_wait(barrier, devices - 1)
    exchange(0, a_send, a_recv, row_tiles, by_fsdp)
    for i in (1, 2, 3):
        loads[i].start()
    loads[0].wait()
    wait_all(recv_sem.at[0], a_recv, row_tiles)
    x_rows = row_tiles * LANES
    x_in = x_buf.at[:, pl.ds(0, x_rows)]
    x_in[...] = gather_features(a_recv, devices, row_tiles)
    qkv_width = w_qkv.shape[1]
    project(x_in, w_qkv, b_send, qkv_width, pitch)
    exchange(1, b_send, b_recv, pitch, by_token)
    for i in (4, 5):
        loads[i].start()
    wait_all(recv_sem.at[1], b_recv, pitch)
    used = qkv_width // LANES
    for d in range(dp_size):
        heads_buf[d * used : (d + 1) * used, :] = sum_block(b_recv, d, pitch, used)

    def turn(values):
        return values * cos_ref[...] + pltpu.roll(values, HD // 2, axis=1) * sin_ref[...]

    group = HEADS // KV_HEADS
    queries = turn(heads_buf[0:HEADS, :]).astype(BF16)
    new_keys = turn(heads_buf[HEADS : HEADS + KV_HEADS, :]).astype(BF16)
    new_values = heads_buf[HEADS + KV_HEADS : HEADS + 2 * KV_HEADS, :].astype(BF16)
    keys_ref[...] = new_keys
    values_ref[...] = new_values
    kv_width = KV_HEADS * HD
    head_of_row = lax.broadcasted_iota(jnp.int32, (HEADS, kv_width), 0) // group
    head_of_lane = lax.broadcasted_iota(jnp.int32, (HEADS, kv_width), 1) // HD
    same_head = head_of_row == head_of_lane
    query_float = queries.astype(F32)
    wide = jnp.concatenate([query_float] * KV_HEADS, axis=1)
    wide = jnp.where(same_head, wide, 0.0).astype(BF16)
    for i in (1, 2):
        loads[i].wait()
    scale = HD ** (-0.5)
    scores = (
        lax.dot_general(
            wide, key_buf[...], (((1,), (1,)), ((), ())), preferred_element_type=F32
        )
        * scale
    )
    position = lax.broadcasted_iota(jnp.int32, scores.shape, 1)
    scores = jnp.where(position < len_ref[0], scores, -1e30)

    def per_query(rows):
        spread = jnp.broadcast_to(rows.astype(F32)[:, None, :], (KV_HEADS, group, HD))
        return spread.reshape(HEADS, HD)

    own_score = jnp.sum(query_float * per_query(new_keys), axis=1, keepdims=True) * scale
    row_max = jnp.maximum(jnp.max(scores, axis=1, keepdims=True), own_score)
    weights = jnp.exp(scores - row_max)
    own_weight = jnp.exp(own_score - row_max)
    denom_sum = jnp.sum(weights, axis=1, keepdims=True) + own_weight
    probability = (weights / denom_sum).astype(BF16)
    own_prob = (own_weight / denom_sum).astype(BF16).astype(F32)
    mixed_wide = jnp.dot(probability, value_buf[...], preferred_element_type=F32)
    mixed_wide = jnp.where(same_head, mixed_wide, 0.0)
    mixed = own_prob * per_query(new_values)
    for h in range(KV_HEADS):
        mixed = mixed + mixed_wide[:, h * HD : (h + 1) * HD]
    c_send[...] = mixed.astype(BF16).astype(F32)
    exchange(2, c_send, c_recv, row_tiles, by_fsdp)
    loads[6].start()
    loads[3].wait()
    wait_all(recv_sem.at[2], c_recv, row_tiles)
    x_in[...] = gather_features(c_recv, devices, row_tiles)
    out_width = w_out.shape[1]
    out_tiles = out_width // LANES
    project(x_in, w_out, d_send, out_width, out_tiles)
    exchange(3, d_send, d_recv, out_tiles, by_token)
    wait_all(recv_sem.at[3], d_recv, out_tiles)
    for d in range(dp_size):
        here = slice(d * out_tiles, (d + 1) * out_tiles)
        mid_buf[here, :] = hid_ref[here, :].astype(F32) + sum_block(
            d_recv, d, out_tiles, out_tiles
        )

    normed_mid = rms_tile(mid_buf[...], mlp_gain_ref[...])
    e_send[...] = normed_mid.astype(BF16).astype(F32)
    mid_tiles = e_recv.shape[0] // devices
    exchange(4, e_send, e_recv, mid_tiles, by_dp)
    loads[4].wait()
    loads[5].wait()
    wait_all(recv_sem.at[4], e_recv, mid_tiles)
    x_buf[...] = gather_features(e_recv, devices, mid_tiles)
    part = w_gate.shape[1] // dp_size

    @pl.loop(1, dp_size + 1)
    def _(step):
        q = lax.rem(my_dp + step, dp_size)
        columns = pl.ds(pl.multiple_of(q * part, LANES), part)
        x = x_buf[...]
        f_send[q, 0] = jnp.dot(x, w_gate[:, columns], preferred_element_type=F32).astype(BF16)
        f_send[q, 1] = jnp.dot(x, w_up[:, columns], preferred_element_type=F32).astype(BF16)

        @pl.when(step < dp_size)
        def _():
            pltpu.make_async_remote_copy(
                src_ref=f_send.at[q],
                dst_ref=f_recv.at[my_dp],
                send_sem=send_sem.at[5],
                recv_sem=recv_sem.at[5],
                device_id=(q, my_fsdp),
                device_id_type=MESH,
            ).start()

    def wait_parts(sem, target):
        whole = target.at[pl.ds(0, dp_size - 1)]
        pltpu.make_async_copy(whole, whole, sem).wait()

    gate_sum = f_send[my_dp, 0].astype(F32)
    up_sum = f_send[my_dp, 1].astype(F32)
    wait_parts(recv_sem.at[5], f_recv)
    for step in range(1, dp_size):
        q = lax.rem(my_dp + step, dp_size)
        gate_sum = gate_sum + f_recv[q, 0].astype(F32)
        up_sum = up_sum + f_recv[q, 1].astype(F32)
    act_buf[my_dp] = (gate_sum / (1.0 + jnp.exp(-gate_sum)) * up_sum).astype(BF16)

    @pl.loop(1, dp_size)
    def _(step):
        q = lax.rem(my_dp + step, dp_size)
        pltpu.make_async_remote_copy(
            src_ref=act_buf.at[my_dp],
            dst_ref=act_buf.at[my_dp],
            send_sem=send_sem.at[6],
            recv_sem=recv_sem.at[6],
            device_id=(q, my_fsdp),
            device_id_type=MESH,
        ).start()

    loads[6].wait()
    wait_parts(recv_sem.at[6], act_buf)
    chunk = 512

    @pl.loop(0, out_width // chunk)
    def _(c):
        columns = pl.ds(pl.multiple_of(c * chunk, chunk), chunk)
        result = None
        for q in range(dp_size):
            piece = jnp.dot(
                act_buf[q], w_down[q * part : (q + 1) * part, columns], preferred_element_type=F32
            )
            result = piece if result is None else result + piece
        for j in range(chunk // LANES):
            row = c * (chunk // LANES) + j
            h_send[pl.ds(row, devices, stride=out_tiles), :] = result[
                :, j * LANES : (j + 1) * LANES
            ]

    exchange(7, h_send, h_recv, out_tiles, by_token)
    wait_all(recv_sem.at[7], h_recv, out_tiles)
    for d in range(dp_size):
        here = slice(d * out_tiles, (d + 1) * out_tiles)
        down = sum_block(h_recv, d, out_tiles, out_tiles)
        hidden_ref[here, :] = (mid_buf[here, :] + down).astype(BF16)

    for phase, (target, rows) in enumerate(
        (
            (a_recv, row_tiles),
            (b_recv, pitch),
            (c_recv, row_tiles),
            (d_recv, out_tiles),
            (e_recv, mid_tiles),
        )
    ):
        wait_all(send_sem.at[phase], target, rows)
    wait_parts(send_sem.at[5], f_send)
    wait_parts(send_sem.at[6], act_buf)
    wait_all(send_sem.at[7], h_recv, out_tiles)


def on_device(
    hidden_in,
    lengths,
    key_cache,
    value_cache,
    attn_gain,
    w_qkv,
    w_out,
    mlp_gain,
    w_gate,
    w_up,
    w_down,
):
    dp_size = lax.axis_size("dp")
    fsdp_size = lax.axis_size("fsdp")
    devices = dp_size * fsdp_size
    seq_count, width = hidden_in.shape
    tile = 8 * LANES
    if (
        seq_count != 1
        or w_qkv.shape[0] % tile
        or w_out.shape[0] != w_qkv.shape[0]
        or w_out.shape[1] % tile
        or w_gate.shape[0] % tile
        or w_gate.shape[1] % (dp_size * LANES)
    ):
        return on_device_plain(
            hidden_in,
            lengths,
            key_cache,
            value_cache,
            attn_gain,
            w_qkv,
            w_out,
            mlp_gain,
            w_gate,
            w_up,
            w_down,
        )
    half = HD // 2
    frequency = rope_base ** (-2.0 * jnp.arange(half, dtype=F32) / HD)
    angles = lengths.astype(F32)[:, None] * frequency[None, :]
    cosine = jnp.cos(angles)
    sine = jnp.sin(angles)
    cosine = jnp.concatenate([cosine, cosine], axis=1)
    sine = jnp.concatenate([-sine, sine], axis=1)
    rows = width // LANES
    context, kv_width = key_cache.shape[1:]
    row_tiles = w_qkv.shape[0] // LANES
    out_tiles = w_out.shape[1] // LANES
    mid_tiles = w_gate.shape[0] // LANES
    pitch = -(-w_qkv.shape[1] // tile) * 8
    part = w_gate.shape[1] // dp_size
    vmem = pl.BlockSpec(memory_space=pltpu.VMEM)
    anyspace = pl.BlockSpec(memory_space=pl.ANY)

    def tiles(count):
        return pltpu.VMEM((count, LANES), F32)

    hidden_out, new_keys, new_values = pl.pallas_call(
        functools.partial(layer_kernel, dp_size, fsdp_size, pitch),
        out_shape=(
            jax.ShapeDtypeStruct((rows, LANES), BF16),
            jax.ShapeDtypeStruct((KV_HEADS, HD), BF16),
            jax.ShapeDtypeStruct((KV_HEADS, HD), BF16),
        ),
        in_specs=[pl.BlockSpec(memory_space=pltpu.SMEM)] + [vmem] * 5 + [anyspace] * 7,
        out_specs=(vmem, vmem, vmem),
        scratch_shapes=[
            pltpu.VMEM(w_qkv.shape, BF16),
            pltpu.VMEM(w_out.shape, BF16),
            pltpu.VMEM(w_gate.shape, BF16),
            pltpu.VMEM(w_up.shape, BF16),
            pltpu.VMEM(w_down.shape, BF16),
            pltpu.VMEM((context, kv_width), BF16),
            pltpu.VMEM((context, kv_width), BF16),
            tiles(rows),
            tiles(devices * row_tiles),
            tiles(devices * pitch),
            tiles(devices * pitch),
            tiles(HEADS + 2 * KV_HEADS),
            tiles(rows),
            tiles(devices * row_tiles),
            tiles(devices * out_tiles),
            tiles(devices * out_tiles),
            tiles(rows),
            tiles(rows),
            tiles(devices * mid_tiles),
            pltpu.VMEM((devices, max(mid_tiles, row_tiles) * LANES), BF16),
            pltpu.VMEM((dp_size, 2, devices, part), BF16),
            pltpu.VMEM((dp_size, 2, devices, part), BF16),
            pltpu.VMEM((dp_size, devices, part), BF16),
            tiles(devices * out_tiles),
            tiles(devices * out_tiles),
            pltpu.SemaphoreType.DMA((7,)),
            pltpu.SemaphoreType.DMA((8,)),
            pltpu.SemaphoreType.DMA((8,)),
        ],
        compiler_params=pltpu.CompilerParams(
            collective_id=0, has_side_effects=True, vmem_limit_bytes=67043328
        ),
    )(
        lengths,
        hidden_in.reshape(rows, LANES),
        cosine,
        sine,
        attn_gain.reshape(rows, LANES),
        mlp_gain.reshape(rows, LANES),
        key_cache,
        value_cache,
        w_qkv,
        w_out,
        w_gate,
        w_up,
        w_down,
    )
    return (hidden_out.reshape(1, width), new_keys.reshape(1, kv_width), new_values.reshape(1, kv_width))


def solution(mesh):
    in_specs = (
        P(("dp", "fsdp"), None),
        P(("dp", "fsdp")),
        P(("dp", "fsdp"), None, None),
        P(("dp", "fsdp"), None, None),
        P(),
        P("fsdp", "dp"),
        P("fsdp", "dp"),
        P(),
        P("dp", "fsdp"),
        P("dp", "fsdp"),
        P("fsdp", "dp"),
    )
    out_specs = (P(("dp", "fsdp"), None), P(("dp", "fsdp"), None), P(("dp", "fsdp"), None))
    return jax.shard_map(
        on_device, mesh=mesh, in_specs=in_specs, out_specs=out_specs, check_vma=False
    )
```

```python
import functools

import jax
import jax.numpy as jnp
from jax import lax
from jax.experimental import pallas as pl
from jax.experimental.pallas import tpu as pltpu
from jax.sharding import PartitionSpec as P

HEADS = 64
KV_HEADS = 8
HD = 128


rope_base = 500000.0
norm_eps = 1e-05


def rms_scale(values, gain_row):
    mean_square = jnp.mean(values * values, axis=-1, keepdims=True)
    return values * lax.rsqrt(mean_square + norm_eps) * gain_row.astype(jnp.float32)


def rotate(values, positions):
    half_dim = values.shape[-1] // 2
    frequency = rope_base ** (-2.0 * jnp.arange(half_dim, dtype=jnp.float32) / values.shape[-1])
    angles = positions.astype(jnp.float32)[:, None] * frequency[None, :]
    cosine = jnp.cos(angles)[:, None, :]
    sine_wave = jnp.sin(angles)[:, None, :]
    lower_half = values[..., :half_dim]
    upper_half = values[..., half_dim:]
    return jnp.concatenate(
        [
            lower_half * cosine - upper_half * sine_wave,
            upper_half * cosine + lower_half * sine_wave,
        ],
        axis=-1,
    )


def attend(queries, new_keys, new_values, key_cache, value_cache, lengths):
    seq_count, context, kv_width = key_cache.shape
    kv_heads = new_keys.shape[1]
    head_dim = new_keys.shape[2]
    score_scale = head_dim ** (-0.5)
    key_rows = key_cache.reshape(seq_count, context, kv_heads, head_dim)
    value_rows = value_cache.reshape(seq_count, context, kv_heads, head_dim)
    grouped = queries.reshape(seq_count, kv_heads, -1, head_dim)
    scores = (
        jnp.einsum("skgd,sckd->skgc", grouped, key_rows, preferred_element_type=jnp.float32)
        * score_scale
    )
    is_valid = (
        jnp.arange(context, dtype=jnp.int32)[None, None, None, :] < lengths[:, None, None, None]
    )
    scores = jnp.where(is_valid, scores, -1e30)
    own_score = (
        jnp.einsum("skgd,skd->skg", grouped, new_keys, preferred_element_type=jnp.float32)
        * score_scale
    )
    row_max = jnp.maximum(jnp.max(scores, axis=-1), own_score)
    weights = jnp.exp(scores - row_max[..., None])
    own_weight = jnp.exp(own_score - row_max)
    denom_sum = jnp.sum(weights, axis=-1) + own_weight
    probability = (weights / denom_sum[..., None]).astype(jnp.bfloat16)
    own_prob = (own_weight / denom_sum).astype(jnp.bfloat16)
    mixed = jnp.einsum(
        "skgc,sckd->skgd", probability, value_rows, preferred_element_type=jnp.float32
    )
    mixed = (
        mixed
        + own_prob.astype(jnp.float32)[..., None] * new_values.astype(jnp.float32)[:, :, None, :]
    )
    return mixed.astype(jnp.bfloat16).reshape(seq_count, -1)


def spread_project(rows, weight):
    block = lax.all_to_all(rows[None], "fsdp", split_axis=2, concat_axis=0, tiled=True)
    block = lax.all_gather(block, "dp", axis=0)
    partial_sum = jnp.einsum("afsk,kn->afsn", block, weight, preferred_element_type=jnp.float32)
    share = lax.psum_scatter(partial_sum, "fsdp", scatter_dimension=1, tiled=True)
    moved = lax.all_to_all(share, "dp", split_axis=0, concat_axis=3, tiled=True)
    return moved[0, 0]


def on_device_plain(
    hidden_in,
    lengths,
    key_cache,
    value_cache,
    attn_gain,
    w_qkv,
    w_out,
    mlp_gain,
    w_gate,
    w_up,
    w_down,
):
    seq_count = hidden_in.shape[0]
    q_width = HEADS * HD
    kv_width = KV_HEADS * HD
    residual = hidden_in.astype(jnp.float32)
    normed = rms_scale(residual, attn_gain).astype(jnp.bfloat16)
    projected = spread_project(normed, w_qkv)
    queries = rotate(projected[:, :q_width].reshape(seq_count, HEADS, HD), lengths).astype(
        jnp.bfloat16
    )
    new_keys = rotate(
        projected[:, q_width : q_width + kv_width].reshape(seq_count, KV_HEADS, HD), lengths
    ).astype(jnp.bfloat16)
    new_values = projected[:, q_width + kv_width :].astype(jnp.bfloat16)
    mixed = attend(
        queries,
        new_keys,
        new_values.reshape(seq_count, KV_HEADS, HD),
        key_cache,
        value_cache,
        lengths,
    )
    attn_sum = spread_project(mixed, w_out)
    residual_mid = residual + attn_sum
    normed_mid = rms_scale(residual_mid, mlp_gain).astype(jnp.bfloat16)
    mlp_in = lax.all_to_all(normed_mid[None], "dp", split_axis=2, concat_axis=0, tiled=True)
    pieces = lax.all_gather(mlp_in[None], "fsdp", axis=0, tiled=True)
    gate_part = jnp.einsum("fask,kn->fasn", pieces, w_gate, preferred_element_type=jnp.float32)
    up_part = jnp.einsum("fask,kn->fasn", pieces, w_up, preferred_element_type=jnp.float32)
    partials = jnp.stack([gate_part, up_part], axis=3)
    summed = lax.psum(partials.astype(jnp.bfloat16), "dp").astype(jnp.float32)
    activated = (jax.nn.silu(summed[:, :, :, 0]) * summed[:, :, :, 1]).astype(jnp.bfloat16)
    reduced_down = lax.psum_scatter(
        jnp.einsum("fask,kn->fasn", activated, w_down, preferred_element_type=jnp.float32),
        "fsdp",
        scatter_dimension=0,
        tiled=True,
    )
    down_sum = lax.all_to_all(
        reduced_down.astype(jnp.bfloat16), "dp", split_axis=1, concat_axis=3, tiled=True
    ).astype(reduced_down.dtype)[0, 0]
    hidden_out = (residual_mid + down_sum).astype(jnp.bfloat16)
    return (hidden_out, new_keys.reshape(seq_count, kv_width), new_values)


LANES = 128
MESH = pl.DeviceIdType.MESH
F32 = jnp.float32
BF16 = jnp.bfloat16


def rms_tile(values, gain):
    total = jnp.sum(jnp.sum(values * values, axis=1, keepdims=True), axis=0, keepdims=True)
    return values * lax.rsqrt(total / values.size + norm_eps) * gain.astype(F32)


def gather_features(ref, stage):
    tokens, rows, _ = ref.shape
    stage[0 : tokens * rows, :] = ref[...].astype(F32).reshape(tokens * rows, LANES)
    pieces = [stage[pl.ds(r, tokens, stride=rows), :] for r in range(rows)]
    return jnp.concatenate(pieces, axis=1).astype(BF16)


def layer_kernel(
    dp_size,
    fsdp_size,
    pitch,
    len_ref,
    hid_ref,
    cos_ref,
    sin_ref,
    attn_gain_ref,
    mlp_gain_ref,
    key_hbm,
    value_hbm,
    qkv_hbm,
    out_hbm,
    gate_hbm,
    up_hbm,
    down_hbm,
    hidden_ref,
    keys_ref,
    values_ref,
    w_qkv,
    w_out,
    w_gate,
    w_up,
    w_down,
    key_buf,
    value_buf,
    a_send,
    a_recv,
    b_send,
    b_recv,
    heads_buf,
    c_send,
    c_recv,
    d_send,
    d_recv,
    mid_buf,
    e_send,
    e_recv,
    x_buf,
    f_send,
    f_recv,
    act_buf,
    h_send,
    h_recv,
    stage,
    total_buf,
    load_sem,
    send_sem,
    recv_sem,
):
    devices = dp_size * fsdp_size
    my_dp = lax.axis_index("dp")
    my_fsdp = lax.axis_index("fsdp")
    me = my_dp * fsdp_size + my_fsdp

    loads = [
        pltpu.make_async_copy(source, target, load_sem.at[i])
        for i, (source, target) in enumerate(
            (
                (qkv_hbm, w_qkv),
                (key_hbm.at[0], key_buf),
                (value_hbm.at[0], value_buf),
                (out_hbm, w_out),
                (gate_hbm, w_gate),
                (up_hbm, w_up),
                (down_hbm, w_down),
            )
        )
    ]
    loads[0].start()

    def place(step):
        other = lax.rem(me + step, devices)
        return other, other // fsdp_size, lax.rem(other, fsdp_size)

    barrier = pltpu.get_barrier_semaphore()

    @pl.loop(1, devices)
    def _(step):
        _, dp_at, fsdp_at = place(step)
        pl.semaphore_signal(barrier, inc=1, device_id=(dp_at, fsdp_at), device_id_type=MESH)

    def exchange(phase, source, target, offset):
        @pl.loop(1, devices)
        def _(step):
            other, dp_at, fsdp_at = place(step)
            pltpu.make_async_remote_copy(
                src_ref=source(offset(other, dp_at, fsdp_at)),
                dst_ref=target(me),
                send_sem=send_sem.at[phase],
                recv_sem=recv_sem.at[phase],
                device_id=(dp_at, fsdp_at),
                device_id_type=MESH,
            ).start()

        own = source(offset(me, my_dp, my_fsdp))
        target(me)[...] = own[...]

    def blocks(ref):
        return lambda i: ref.at[i]

    def runs(ref, rows):
        return lambda i: ref.at[pl.ds(pl.multiple_of(i * rows, 8), rows)]

    def wait_all(sem, target, rows):
        whole = target.at[pl.ds(0, (devices - 1) * rows)]
        pltpu.make_async_copy(whole, whole, sem).wait()

    def by_fsdp(other, dp_at, fsdp_at):
        return fsdp_at

    def by_dp(other, dp_at, fsdp_at):
        return dp_at

    def by_token(other, dp_at, fsdp_at):
        return other

    def project(x, weight, target, width, step_pitch):
        chunk = 512

        @pl.loop(0, width // chunk)
        def _(c):
            columns = pl.ds(pl.multiple_of(c * chunk, chunk), chunk)
            result = jnp.dot(x[...], weight[:, columns], preferred_element_type=F32)
            for j in range(chunk // LANES):
                row = c * (chunk // LANES) + j
                target[pl.ds(row, devices, stride=step_pitch), :] = result[
                    :, j * LANES : (j + 1) * LANES
                ]

    def sum_parts(ref, dp_at):
        total = None
        for f in range(fsdp_size):
            piece = ref[dp_at * fsdp_size + f].astype(F32)
            total = piece if total is None else total + piece
        return total

    def sum_block(ref, dp_at, rows, used):
        total = None
        for f in range(fsdp_size):
            start = (dp_at * fsdp_size + f) * rows
            piece = ref[start : start + used, :]
            total = piece if total is None else total + piece
        return total

    residual = hid_ref[...].astype(F32)
    normed = rms_tile(residual, attn_gain_ref[...])
    a_send[...] = normed.astype(BF16).reshape(a_send.shape)
    row_tiles = a_recv.shape[1]
    pl.semaphore_wait(barrier, devices - 1)
    exchange(0, blocks(a_send), blocks(a_recv), by_fsdp)
    for i in (1, 2, 3):
        loads[i].start()
    loads[0].wait()
    wait_all(recv_sem.at[0], a_recv, 1)
    x_rows = row_tiles * LANES
    x_in = x_buf.at[:, pl.ds(0, x_rows)]
    x_in[...] = gather_features(a_recv, stage)
    qkv_width = w_qkv.shape[1]
    project(x_in, w_qkv, b_send, qkv_width, pitch)
    exchange(1, runs(b_send, pitch), runs(b_recv, pitch), by_token)
    for i in (4, 5):
        loads[i].start()
    wait_all(recv_sem.at[1], b_recv, pitch)
    used = qkv_width // LANES
    for d in range(dp_size):
        heads_buf[d * used : (d + 1) * used, :] = sum_block(b_recv, d, pitch, used)

    def turn(values):
        return values * cos_ref[...] + pltpu.roll(values, HD // 2, axis=1) * sin_ref[...]

    group = HEADS // KV_HEADS
    queries = turn(heads_buf[0:HEADS, :]).astype(BF16)
    new_keys = turn(heads_buf[HEADS : HEADS + KV_HEADS, :]).astype(BF16)
    new_values = heads_buf[HEADS + KV_HEADS : HEADS + 2 * KV_HEADS, :].astype(BF16)
    keys_ref[...] = new_keys
    values_ref[...] = new_values
    kv_width = KV_HEADS * HD
    head_of_row = lax.broadcasted_iota(jnp.int32, (HEADS, kv_width), 0) // group
    head_of_lane = lax.broadcasted_iota(jnp.int32, (HEADS, kv_width), 1) // HD
    same_head = head_of_row == head_of_lane
    query_float = queries.astype(F32)
    wide = jnp.concatenate([query_float] * KV_HEADS, axis=1)
    wide = jnp.where(same_head, wide, 0.0).astype(BF16)
    for i in (1, 2):
        loads[i].wait()
    scale = HD ** (-0.5)
    scores = (
        lax.dot_general(
            wide, key_buf[...], (((1,), (1,)), ((), ())), preferred_element_type=F32
        )
        * scale
    )
    position = lax.broadcasted_iota(jnp.int32, scores.shape, 1)
    scores = jnp.where(position < len_ref[0], scores, -1e30)

    def per_query(rows):
        spread = jnp.broadcast_to(rows.astype(F32)[:, None, :], (KV_HEADS, group, HD))
        return spread.reshape(HEADS, HD)

    own_score = jnp.sum(query_float * per_query(new_keys), axis=1, keepdims=True) * scale
    row_max = jnp.maximum(jnp.max(scores, axis=1, keepdims=True), own_score)
    weights = jnp.exp(scores - row_max)
    own_weight = jnp.exp(own_score - row_max)
    denom_sum = jnp.sum(weights, axis=1, keepdims=True) + own_weight
    probability = (weights / denom_sum).astype(BF16)
    own_prob = (own_weight / denom_sum).astype(BF16).astype(F32)
    mixed_wide = jnp.dot(probability, value_buf[...], preferred_element_type=F32)
    mixed_wide = jnp.where(same_head, mixed_wide, 0.0)
    mixed = own_prob * per_query(new_values)
    for h in range(KV_HEADS):
        mixed = mixed + mixed_wide[:, h * HD : (h + 1) * HD]
    c_send[...] = mixed.astype(BF16).reshape(c_send.shape)
    exchange(2, blocks(c_send), blocks(c_recv), by_fsdp)
    loads[6].start()
    loads[3].wait()
    wait_all(recv_sem.at[2], c_recv, 1)
    x_in[...] = gather_features(c_recv, stage)
    out_width = w_out.shape[1]
    out_tiles = out_width // LANES
    project(x_in, w_out, stage, out_width, out_tiles)
    d_send[...] = stage[0 : devices * out_tiles, :].reshape(d_send.shape).astype(BF16)
    exchange(3, blocks(d_send), blocks(d_recv), by_token)
    wait_all(recv_sem.at[3], d_recv, 1)
    for d in range(dp_size):
        here = slice(d * out_tiles, (d + 1) * out_tiles)
        mid_buf[here, :] = hid_ref[here, :].astype(F32) + sum_parts(d_recv, d)

    normed_mid = rms_tile(mid_buf[...], mlp_gain_ref[...])
    e_send[...] = normed_mid.astype(BF16).reshape(e_send.shape)
    exchange(4, blocks(e_send), blocks(e_recv), by_dp)
    loads[4].wait()
    loads[5].wait()
    wait_all(recv_sem.at[4], e_recv, 1)
    x_buf[...] = gather_features(e_recv, stage)
    part = w_gate.shape[1] // dp_size

    @pl.loop(1, dp_size + 1)
    def _(step):
        q = lax.rem(my_dp + step, dp_size)
        columns = pl.ds(pl.multiple_of(q * part, LANES), part)
        x = x_buf[...]
        f_send[q, 0] = jnp.dot(x, w_gate[:, columns], preferred_element_type=F32).astype(BF16)
        f_send[q, 1] = jnp.dot(x, w_up[:, columns], preferred_element_type=F32).astype(BF16)

        @pl.when(step < dp_size)
        def _():
            pltpu.make_async_remote_copy(
                src_ref=f_send.at[q],
                dst_ref=f_recv.at[my_dp],
                send_sem=send_sem.at[5],
                recv_sem=recv_sem.at[5],
                device_id=(q, my_fsdp),
                device_id_type=MESH,
            ).start()

    def wait_parts(sem, target):
        whole = target.at[pl.ds(0, dp_size - 1)]
        pltpu.make_async_copy(whole, whole, sem).wait()

    gate_sum = f_send[my_dp, 0].astype(F32)
    up_sum = f_send[my_dp, 1].astype(F32)
    wait_parts(recv_sem.at[5], f_recv)
    for step in range(1, dp_size):
        q = lax.rem(my_dp + step, dp_size)
        gate_sum = gate_sum + f_recv[q, 0].astype(F32)
        up_sum = up_sum + f_recv[q, 1].astype(F32)
    act_buf[my_dp] = (gate_sum / (1.0 + jnp.exp(-gate_sum)) * up_sum).astype(BF16)

    @pl.loop(1, dp_size)
    def _(step):
        q = lax.rem(my_dp + step, dp_size)
        pltpu.make_async_remote_copy(
            src_ref=act_buf.at[my_dp],
            dst_ref=act_buf.at[my_dp],
            send_sem=send_sem.at[6],
            recv_sem=recv_sem.at[7 + step],
            device_id=(q, my_fsdp),
            device_id_type=MESH,
        ).start()

    loads[6].wait()
    chunk = 512
    for step in range(dp_size):
        source = lax.rem(my_dp - step + dp_size, dp_size)
        if step:
            block = act_buf.at[0]
            pltpu.make_async_copy(block, block, recv_sem.at[7 + step]).wait()
        first, last = step == 0, step == dp_size - 1
        part_rows = pl.ds(pl.multiple_of(source * part, LANES), part)

        @pl.loop(0, out_width // chunk)
        def _(c):
            columns = pl.ds(pl.multiple_of(c * chunk, chunk), chunk)
            result = jnp.dot(
                act_buf[source], w_down[part_rows, columns], preferred_element_type=F32
            )
            if not first:
                result = result + total_buf[c]
            if not last:
                total_buf[c] = result
            else:
                for j in range(chunk // LANES):
                    row = c * (chunk // LANES) + j
                    stage[pl.ds(row, devices, stride=out_tiles), :] = result[
                        :, j * LANES : (j + 1) * LANES
                    ]

    h_send[...] = stage[0 : devices * out_tiles, :].reshape(h_send.shape).astype(BF16)
    exchange(7, blocks(h_send), blocks(h_recv), by_token)
    wait_all(recv_sem.at[7], h_recv, 1)
    for d in range(dp_size):
        here = slice(d * out_tiles, (d + 1) * out_tiles)
        down = sum_parts(h_recv, d)
        hidden_ref[here, :] = (mid_buf[here, :] + down).astype(BF16)

    for phase, (target, rows) in enumerate(
        (
            (a_recv, 1),
            (b_recv, pitch),
            (c_recv, 1),
            (d_recv, 1),
            (e_recv, 1),
        )
    ):
        wait_all(send_sem.at[phase], target, rows)
    wait_parts(send_sem.at[5], f_send)
    wait_parts(send_sem.at[6], act_buf)
    wait_all(send_sem.at[7], h_recv, 1)


def on_device(
    hidden_in,
    lengths,
    key_cache,
    value_cache,
    attn_gain,
    w_qkv,
    w_out,
    mlp_gain,
    w_gate,
    w_up,
    w_down,
):
    dp_size = lax.axis_size("dp")
    fsdp_size = lax.axis_size("fsdp")
    devices = dp_size * fsdp_size
    seq_count, width = hidden_in.shape
    tile = 8 * LANES
    if (
        seq_count != 1
        or w_qkv.shape[0] % tile
        or w_out.shape[0] != w_qkv.shape[0]
        or w_out.shape[1] % tile
        or w_gate.shape[0] % tile
        or w_gate.shape[1] % (dp_size * LANES)
    ):
        return on_device_plain(
            hidden_in,
            lengths,
            key_cache,
            value_cache,
            attn_gain,
            w_qkv,
            w_out,
            mlp_gain,
            w_gate,
            w_up,
            w_down,
        )
    half = HD // 2
    frequency = rope_base ** (-2.0 * jnp.arange(half, dtype=F32) / HD)
    angles = lengths.astype(F32)[:, None] * frequency[None, :]
    cosine = jnp.cos(angles)
    sine = jnp.sin(angles)
    cosine = jnp.concatenate([cosine, cosine], axis=1)
    sine = jnp.concatenate([-sine, sine], axis=1)
    rows = width // LANES
    context, kv_width = key_cache.shape[1:]
    row_tiles = w_qkv.shape[0] // LANES
    out_tiles = w_out.shape[1] // LANES
    mid_tiles = w_gate.shape[0] // LANES
    pitch = -(-w_qkv.shape[1] // tile) * 8
    part = w_gate.shape[1] // dp_size
    vmem = pl.BlockSpec(memory_space=pltpu.VMEM)
    anyspace = pl.BlockSpec(memory_space=pl.ANY)

    def tiles(count):
        return pltpu.VMEM((count, LANES), F32)

    def blocks(count, height):
        return pltpu.VMEM((count, height, LANES), BF16)

    hidden_out, new_keys, new_values = pl.pallas_call(
        functools.partial(layer_kernel, dp_size, fsdp_size, pitch),
        out_shape=(
            jax.ShapeDtypeStruct((rows, LANES), BF16),
            jax.ShapeDtypeStruct((KV_HEADS, HD), BF16),
            jax.ShapeDtypeStruct((KV_HEADS, HD), BF16),
        ),
        in_specs=[pl.BlockSpec(memory_space=pltpu.SMEM)] + [vmem] * 5 + [anyspace] * 7,
        out_specs=(vmem, vmem, vmem),
        scratch_shapes=[
            pltpu.VMEM(w_qkv.shape, BF16),
            pltpu.VMEM(w_out.shape, BF16),
            pltpu.VMEM(w_gate.shape, BF16),
            pltpu.VMEM(w_up.shape, BF16),
            pltpu.VMEM(w_down.shape, BF16),
            pltpu.VMEM((context, kv_width), BF16),
            pltpu.VMEM((context, kv_width), BF16),
            blocks(fsdp_size, row_tiles),
            blocks(devices, row_tiles),
            tiles(devices * pitch),
            tiles(devices * pitch),
            tiles(HEADS + 2 * KV_HEADS),
            blocks(fsdp_size, row_tiles),
            blocks(devices, row_tiles),
            blocks(devices, out_tiles),
            blocks(devices, out_tiles),
            tiles(rows),
            blocks(dp_size, mid_tiles),
            blocks(devices, mid_tiles),
            pltpu.VMEM((devices, max(mid_tiles, row_tiles) * LANES), BF16),
            pltpu.VMEM((dp_size, 2, devices, part), BF16),
            pltpu.VMEM((dp_size, 2, devices, part), BF16),
            pltpu.VMEM((dp_size, devices, part), BF16),
            blocks(devices, out_tiles),
            blocks(devices, out_tiles),
            tiles(devices * max(row_tiles, mid_tiles, out_tiles)),
            pltpu.VMEM((out_tiles // 4, devices, 4 * LANES), F32),
            pltpu.SemaphoreType.DMA((7,)),
            pltpu.SemaphoreType.DMA((8,)),
            pltpu.SemaphoreType.DMA((8 + dp_size,)),
        ],
        compiler_params=pltpu.CompilerParams(
            collective_id=0, has_side_effects=True, vmem_limit_bytes=67043328
        ),
    )(
        lengths,
        hidden_in.reshape(rows, LANES),
        cosine,
        sine,
        attn_gain.reshape(rows, LANES),
        mlp_gain.reshape(rows, LANES),
        key_cache,
        value_cache,
        w_qkv,
        w_out,
        w_gate,
        w_up,
        w_down,
    )
    return (hidden_out.reshape(1, width), new_keys.reshape(1, kv_width), new_values.reshape(1, kv_width))


def solution(mesh):
    in_specs = (
        P(("dp", "fsdp"), None),
        P(("dp", "fsdp")),
        P(("dp", "fsdp"), None, None),
        P(("dp", "fsdp"), None, None),
        P(),
        P("fsdp", "dp"),
        P("fsdp", "dp"),
        P(),
        P("dp", "fsdp"),
        P("dp", "fsdp"),
        P("fsdp", "dp"),
    )
    out_specs = (P(("dp", "fsdp"), None), P(("dp", "fsdp"), None), P(("dp", "fsdp"), None))
    return jax.shard_map(
        on_device, mesh=mesh, in_specs=in_specs, out_specs=out_specs, check_vma=False
    )
```
